32 devices in a mesh: grow: 16 (over z, y, core), trans: 2 (over x).
Axes of the slice: x: 2, y: 2, z: 4, core: 2. Of those that a mesh axis runs over, the one named last changes fastest.
Arguments:
- phase_label: int32 [384, 16, 128], P('grow', 'trans'), may hold values from 0 to 3
- grain_label: int32 [384, 16, 128], P('grow', 'trans'), may hold values from 0 to 31
- grain_orient: int32 [32], replicated, may hold values from 0 to 7
- orient_mobility: float32 [8], replicated, may hold values from 0.4 to 1.2
- solute_init: float32 [2, 384, 16, 128], P(None, 'grow', 'trans'), may hold values from 0.1 to 0.5
- partition: float32 [4, 2], replicated, may hold values from -0.5 to 0.5
Outputs:
- phase_out: float32 [4, 384, 16, 128], P(None, 'grow', 'trans')
- solute_out: float32 [2, 384, 16, 128], P(None, 'grow', 'trans')
The draws below stay inside these ranges and needn't reach their ends.
All inputs are finite; a program needn't handle non-finite values.
Results may differ from the reference program's by a relative error of at most 0.00002.
Values sent between devices are 32-bit elements; how exact they have to be, the bound alone decides.
No kernel may reach another device: no remote copies, remote signals or barrier semaphores. Data moves between devices by JAX's collectives and lax.ppermute only.
A program may use at most 64 MiB of HBM per device.

```python
import math
import jax
import jax.numpy as jnp

COLUMNS = 128
SHIFT = 16
PHASES = 4
SOLUTES = 2
GRAINS = 32
ORIENTS = 8
DEPTH = 384
BREADTH = 16


def touch_ends(entries, own_key, least, top_value):
    longest = entries.shape.index(max(entries.shape))
    spots = []
    for shift in (0, 1):
        where = [jax.random.randint(jax.random.fold_in(own_key, axis), (), 0, length) for axis, length in enumerate(entries.shape)]
        where[longest] = (where[longest] + shift) % entries.shape[longest]
        spots.append(tuple(where))
    return entries.at[spots[0]].set(least).at[spots[1]].set(top_value)


def steps_of(own_key, shape, cuts, low, largest):
    loudness, own = 1.0, jax.random.fold_in(own_key, 6)
    for position, parts in cuts:
        steps = jnp.exp(jax.random.uniform(jax.random.fold_in(own, position), (parts,), jnp.float32, low / len(cuts), largest / len(cuts)))
        loudness = loudness * jnp.repeat(steps, shape[position] // parts).reshape([-1 if axis == position else 1 for axis in range(len(shape))])
    return loudness


def setup_inputs(seed: int = 0) -> dict:
    arg_keys = jax.random.split(jax.random.key(seed), 7)
    phase_label = touch_ends(jax.random.randint(arg_keys[0], (DEPTH, BREADTH, COLUMNS), 0, PHASES), jax.random.fold_in(arg_keys[0], 1), 0, PHASES - 1).astype(jnp.int32)
    grain_label = touch_ends(jax.random.randint(arg_keys[1], (DEPTH, BREADTH, COLUMNS), 0, GRAINS), jax.random.fold_in(arg_keys[1], 1), 0, GRAINS - 1).astype(jnp.int32)
    grain_orient = touch_ends(jax.random.randint(arg_keys[2], (GRAINS,), 0, ORIENTS), jax.random.fold_in(arg_keys[2], 1), 0, ORIENTS - 1).astype(jnp.int32)
    orient_mobility = jnp.clip(jnp.exp(jax.random.uniform(arg_keys[3], (ORIENTS,), jnp.float32, math.log(0.4), math.log(1.2))), 0.4, 1.2)
    solute_init = jnp.clip(0.1 + 0.4 * jax.random.uniform(arg_keys[4], (SOLUTES, DEPTH, BREADTH, COLUMNS), jnp.float32) ** steps_of(arg_keys[4], (SOLUTES, DEPTH, BREADTH, COLUMNS), ((1, 16), (2, 2)), -0.2, 0.2), 0.1, 0.5)
    partition = jnp.clip(jax.random.uniform(arg_keys[5], (PHASES, SOLUTES), jnp.float32, -0.5, 0.5), -0.5, 0.5)
    return dict(phase_label=phase_label, grain_label=grain_label, grain_orient=grain_orient, orient_mobility=orient_mobility, solute_init=solute_init, partition=partition)


ANISOTROPY = 1.5
WELL_HEIGHT = 4.0
TIME_STEP = 0.06
LIQUID_DIFFUSION = 1.0
SOLID_DIFFUSION = 0.1
COOLING_WEIGHTS = (-1.0, 0.8, 0.7, 0.6)
FIRST_WEIGHTS = (0.5, -1.0, 0.4, 0.3)
SECOND_WEIGHTS = (0.4, 0.3, -1.0, 0.5)
INFLOW_FIRST = 0.3
INFLOW_SECOND = 0.2
LIQUID_MOBILITY = 1.0


def advance(padded, mobility, undercool, partition):
    centre = padded[:, 1:-1, 1:-1]
    plane_up = padded[:, 2:, 1:-1]
    plane_down = padded[:, :-2, 1:-1]
    row_next = padded[:, 1:-1, 2:]
    row_prev = padded[:, 1:-1, :-2]
    col_next = jnp.roll(centre, -1, axis=3)
    col_prev = jnp.roll(centre, 1, axis=3)
    phases = centre[:4]
    solutes = centre[4:]
    laplace = ANISOTROPY * (plane_up[:4] + plane_down[:4] - 2.0 * phases)
    laplace = laplace + (row_next[:4] + row_prev[:4] - 2.0 * phases)
    laplace = laplace + (col_next[:4] + col_prev[:4] - 2.0 * phases)
    cooling_w = jnp.array(COOLING_WEIGHTS, dtype=phases.dtype).reshape(4, 1, 1, 1)
    first_w = jnp.array(FIRST_WEIGHTS, dtype=phases.dtype).reshape(4, 1, 1, 1)
    second_w = jnp.array(SECOND_WEIGHTS, dtype=phases.dtype).reshape(4, 1, 1, 1)
    driving = cooling_w * undercool[None] + first_w * solutes[0][None] + second_w * solutes[1][None]
    forcing = laplace + WELL_HEIGHT * phases * (1.0 - phases) * (phases - 0.5 + driving)
    growth_rate = mobility[None] * (forcing - jnp.mean(forcing, axis=0, keepdims=True))
    trials = jnp.clip(phases + TIME_STEP * growth_rate, 0.0, 1.0)
    new_phases = trials / jnp.sum(trials, axis=0, keepdims=True)
    own_diffusion = SOLID_DIFFUSION + (LIQUID_DIFFUSION - SOLID_DIFFUSION) * centre[0]
    influx = jnp.zeros_like(solutes)
    for neighbour in (plane_up, plane_down, row_next, row_prev, col_next, col_prev):
        other = SOLID_DIFFUSION + (LIQUID_DIFFUSION - SOLID_DIFFUSION) * neighbour[0]
        influx = influx + 0.5 * (other + own_diffusion)[None] * (neighbour[4:] - solutes)
    changes = new_phases - phases
    rejected = partition[0][:, None, None, None] * changes[0][None]
    rejected = rejected + partition[1][:, None, None, None] * changes[1][None]
    rejected = rejected + partition[2][:, None, None, None] * changes[2][None]
    rejected = rejected + partition[3][:, None, None, None] * changes[3][None]
    new_solutes = solutes + TIME_STEP * influx - rejected
    return jnp.concatenate([new_phases, new_solutes], axis=0)


def pad_grid(fields):
    padded = jnp.concatenate([fields[:, :1], fields, fields[:, -1:]], axis=1)
    return jnp.concatenate([padded[:, :, -1:], padded, padded[:, :, :1]], axis=2)


def cooling(heights, total_depth):
    return (2.0 * (0.5 - (heights + 0.5) / total_depth))[:, None, None]


def reference(phase_label, grain_label, grain_orient, orient_mobility, solute_init, partition):
    grain_mobility = orient_mobility[grain_orient]
    mobility = grain_mobility[grain_label]
    labels = jnp.arange(4, dtype=jnp.int32)[:, None, None, None]
    phases = (phase_label[None] == labels).astype(solute_init.dtype)
    fields = jnp.concatenate([phases, solute_init], axis=0)
    total_depth = fields.shape[1]
    heights = jnp.arange(total_depth, dtype=jnp.int32).astype(fields.dtype)
    undercool = cooling(heights, total_depth)
    fields = advance(pad_grid(fields), mobility, undercool, partition)
    fields = advance(pad_grid(fields), mobility, undercool, partition)
    inflow = jnp.array([1.0, 0.0, 0.0, 0.0, INFLOW_FIRST, INFLOW_SECOND], dtype=fields.dtype)
    liquid = inflow[:, None, None, None] * jnp.ones((6, SHIFT, fields.shape[2], fields.shape[3]), fields.dtype)
    fields = jnp.concatenate([fields[:, SHIFT:], liquid], axis=1)
    liquid_mob = LIQUID_MOBILITY * jnp.ones((SHIFT, fields.shape[2], fields.shape[3]), fields.dtype)
    mobility = jnp.concatenate([mobility[SHIFT:], liquid_mob], axis=0)
    fields = advance(pad_grid(fields), mobility, undercool, partition)
    return fields[:4], fields[4:]
```

```python
import functools

import jax
import jax.numpy as jnp
from jax import lax
from jax.experimental import pallas as pl
from jax.experimental.pallas import tpu as pltpu
from jax.sharding import PartitionSpec as P

SHIFT = 16
STEPS = 3

PHASES = 4
SOLUTES = 2
FIELDS = PHASES + SOLUTES
RAW = 4

ANISOTROPY = 1.5
WELL_HEIGHT = 4.0
TIME_STEP = 0.06
LIQUID_DIFFUSION = 1.0
SOLID_DIFFUSION = 0.1
COOLING_WEIGHTS = (-1.0, 0.8, 0.7, 0.6)
FIRST_WEIGHTS = (0.5, -1.0, 0.4, 0.3)
SECOND_WEIGHTS = (0.4, 0.3, -1.0, 0.5)
INFLOW = (1.0, 0.0, 0.0, 0.0, 0.3, 0.2)
LIQUID_MOBILITY = 1.0

F32 = jnp.float32


class Plan:
    def __init__(self, planes, rows, slabs, blocks):
        self.planes, self.rows, self.slabs, self.blocks = planes, rows, slabs, blocks
        self.own = planes - SHIFT + STEPS
        self.next = SHIFT + STEPS
        self.depth = self.own + self.next
        self.pitch = (rows + 2 * STEPS) | 1
        self.window_rows = -(-self.depth * self.pitch // 8) * 8
        self.own_pieces, self.own_rows = self.pieces(0, self.own)
        self.next_pieces, self.next_rows = self.pieces(self.own, self.depth)

    def pieces(self, first, last):
        found, lengths = [], []
        for side in range(2):
            if self.blocks > 2 or not lengths:
                lengths.append(0)
            for j in range(first, last):
                for array in range(RAW):
                    inset = 1 if array == 3 else 0
                    count = min(STEPS - inset, j - inset, self.depth - 1 - inset - j)
                    if count > 0:
                        found.append((side, array, j, count, len(lengths) - 1, lengths[-1]))
                        lengths[-1] += count
        return found, [-(-length // 8) * 8 for length in lengths]


def pack_kernel(plan, phase, grain, solutes, orient, mobil, own, grow, *halos):
    rows = plan.rows
    table = jnp.zeros((rows, 128), F32)
    lanes = lax.broadcasted_iota(jnp.int32, (rows, 128), 1)
    for g in range(orient.shape[0]):
        table = jnp.where(lanes == g, mobil[orient[g]], table)
    own_halos = halos[: len(plan.own_rows)]
    next_halos = halos[len(plan.own_rows) :]
    first = SHIFT - STEPS
    where = {}
    for pieces, buffers, shift in ((plan.own_pieces, own_halos, first), (plan.next_pieces, next_halos, -plan.own)):
        for side, array, j, count, buffer, offset in pieces:
            where.setdefault((array, j + shift), []).append((side, count, buffers[buffer], offset))
    for z in range(plan.planes):
        label = phase[z].astype(F32)
        mobility = jnp.take_along_axis(table, grain[z], axis=1)
        for array, tile in enumerate((label, solutes[0, z], solutes[1, z], mobility)):
            if z >= first:
                own[array, z - first] = tile
            if z < plan.next:
                grow[array, z] = tile
            for side, count, buffer, offset in where.get((array, z), ()):
                piece = tile[:count] if side == 0 else tile[rows - count :]
                buffer[offset : offset + count, :] = piece


def step_tile(load, undercool, mobility, partition):
    centre = [load(f, 0, 0) for f in range(FIELDS)]
    below = [load(f, -1, 0) for f in range(FIELDS)]
    above = [load(f, 1, 0) for f in range(FIELDS)]
    prev = [load(f, 0, -1) for f in range(FIELDS)]
    after = [load(f, 0, 1) for f in range(FIELDS)]
    left = [pltpu.roll(c, 1, 1) for c in centre]
    right = [pltpu.roll(c, c.shape[1] - 1, 1) for c in centre]
    c0, c1 = centre[4], centre[5]
    forcing = []
    for a in range(PHASES):
        p = centre[a]
        laplace = ANISOTROPY * (above[a] + below[a]) + ((prev[a] + after[a]) + (left[a] + right[a]))
        laplace = laplace - (2.0 * ANISOTROPY + 4.0) * p
        driving = (COOLING_WEIGHTS[a] * undercool - 0.5) + FIRST_WEIGHTS[a] * c0 + SECOND_WEIGHTS[a] * c1
        well = WELL_HEIGHT * p
        forcing.append(laplace + (well - well * p) * (p + driving))
    mean = 0.25 * ((forcing[0] + forcing[1]) + (forcing[2] + forcing[3]))
    rate = TIME_STEP * mobility
    trials = [jnp.clip(centre[a] + rate * (forcing[a] - mean), 0.0, 1.0) for a in range(PHASES)]
    scale = 1.0 / ((trials[0] + trials[1]) + (trials[2] + trials[3]))
    phases = [t * scale for t in trials]
    slope = 0.5 * TIME_STEP * (LIQUID_DIFFUSION - SOLID_DIFFUSION)
    base = 0.5 * TIME_STEP * 2.0 * SOLID_DIFFUSION
    own = slope * centre[0] + base
    inflow = [None, None]
    for side in (above, below, prev, after, left, right):
        both = slope * side[0] + own
        for k in range(SOLUTES):
            flux = both * (side[4 + k] - centre[4 + k])
            inflow[k] = flux if inflow[k] is None else inflow[k] + flux
    changes = [phases[a] - centre[a] for a in range(PHASES)]
    solutes = []
    for k in range(SOLUTES):
        rejected = (partition[0, k] * changes[0] + partition[1, k] * changes[1]) + (
            partition[2, k] * changes[2] + partition[3, k] * changes[3]
        )
        solutes.append(centre[4 + k] + (inflow[k] - rejected))
    return phases + solutes


def main_kernel(plan, own, grow, partition, *refs):
    n_own, n_next = len(plan.own_rows), len(plan.next_rows)
    own_halos, next_halos = refs[:n_own], refs[n_own : n_own + n_next]
    phase_out, solute_out, field_a, field_b, mob, result, sems = refs[n_own + n_next :]
    rows, pitch, depth = plan.rows, plan.pitch, plan.depth
    slab = lax.axis_index("grow")
    first_slab, last_slab = slab == 0, slab == plan.slabs - 1
    edge = plan.own - 1
    total = plan.planes * plan.slabs

    def put(array, j, row, count, tile):
        spot = pl.ds(j * pitch + row, count)
        if array == 0:
            for a in range(PHASES):
                field_a[a, spot, :] = jnp.where(tile == a, 1.0, 0.0)
        elif array == 3:
            mob[spot, :] = tile
        else:
            field_a[PHASES - 1 + array, spot, :] = tile

    for j in range(depth):
        for array in range(RAW):
            tile = own[array, j] if j < plan.own else grow[array, j - plan.own]
            put(array, j, STEPS, rows, tile)
    for pieces, buffers in ((plan.own_pieces, own_halos), (plan.next_pieces, next_halos)):
        for side, array, j, count, buffer, offset in pieces:
            row = STEPS + rows if side == 0 else STEPS - count
            put(array, j, row, count, buffers[buffer][offset : offset + count, :])

    def repeat_edge(fields, source, target):
        for f in range(FIELDS):
            for row in (0, pitch - 8):
                fields[f, pl.ds(target * pitch + row, 8), :] = fields[f, pl.ds(source * pitch + row, 8), :]

    def sweep(source, target, begin, end, starts, base, mob_shift):
        def body(j, carry):
            height = (base + j).astype(F32)
            undercool = 2.0 * (0.5 - (height + 0.5) * (1.0 / total))
            for start in starts:
                at = j * pitch + start

                def load(f, dz, dr):
                    return source[f, pl.ds(at + dz * pitch + dr, 8), :]

                new = step_tile(load, undercool, mob[pl.ds(at, 8), :], partition)
                if target is None:
                    for f in range(FIELDS):
                        result[f, j - STEPS] = new[f]
                else:
                    for f in range(FIELDS):
                        target[f, pl.ds(at, 8), :] = new[f]
            return carry

        lax.fori_loop(begin, end, body, 0)

    origin = slab * plan.planes + SHIFT - STEPS

    @pl.when(last_slab)
    def _():
        repeat_edge(field_a, edge, edge + 1)

    sweep(field_a, field_b, 1, depth - 1, (1, rows + 2 * STEPS - 9), origin, 0)

    @pl.when(last_slab)
    def _():
        repeat_edge(field_b, edge, edge + 1)

    sweep(field_b, field_a, 2, depth - 2, (2, rows + 2 * STEPS - 10), origin, 0)

    @pl.when(last_slab)
    def _():
        for j in range(edge + 1, depth - 2):
            for row in (0, pitch - 8):
                spot = pl.ds(j * pitch + row, 8)
                for f in range(FIELDS):
                    field_a[f, spot, :] = jnp.full((8, 128), INFLOW[f], F32)
                mob[spot, :] = jnp.full((8, 128), LIQUID_MOBILITY, F32)

    @pl.when(first_slab)
    def _():
        repeat_edge(field_a, STEPS, STEPS - 1)

    sweep(field_a, None, STEPS, depth - STEPS, (STEPS,), slab * plan.planes - STEPS, 0)
    copies = (
        pltpu.make_async_copy(result.at[pl.ds(0, PHASES)], phase_out, sems.at[0]),
        pltpu.make_async_copy(result.at[pl.ds(PHASES, SOLUTES)], solute_out, sems.at[1]),
    )
    for copy in copies:
        copy.start()
    for copy in copies:
        copy.wait()


def shards(phase_label, grain_label, grain_orient, orient_mobility, solute_init, partition):
    slabs, blocks = lax.axis_size("grow"), lax.axis_size("trans")
    planes, rows, columns = phase_label.shape
    plan = Plan(planes, rows, slabs, blocks)
    vmem, smem, hbm = (pl.BlockSpec(memory_space=m) for m in (pltpu.VMEM, pltpu.SMEM, pl.ANY))
    halo_shapes = [
        jax.ShapeDtypeStruct((length, columns), F32) for length in plan.own_rows + plan.next_rows
    ]
    own, grow, *halos = pl.pallas_call(
        functools.partial(pack_kernel, plan),
        out_shape=[
            jax.ShapeDtypeStruct((RAW, plan.own, rows, columns), F32),
            jax.ShapeDtypeStruct((RAW, plan.next, rows, columns), F32),
            *halo_shapes,
        ],
        in_specs=[vmem, vmem, vmem, smem, smem],
        out_specs=[vmem] * (2 + len(halo_shapes)),
        name="pack",
    )(phase_label, grain_label, solute_init, grain_orient, orient_mobility)

    ups = [(b + 1) % blocks for b in range(blocks)]
    downs = [(b - 1) % blocks for b in range(blocks)]

    def fetch(value, side, hop):
        others = ups if side == 0 else downs
        pairs = [
            ((s + hop) * blocks + others[b], s * blocks + b) for s in range(slabs - hop) for b in range(blocks)
        ]
        return lax.ppermute(value, ("grow", "trans"), pairs)

    n_own = len(plan.own_rows)
    own_halos = [fetch(value, side, 0) for side, value in enumerate(halos[:n_own])]
    next_halos = [fetch(value, side, 1) for side, value in enumerate(halos[n_own:])]
    received = lax.ppermute(grow, "grow", [(s + 1, s) for s in range(slabs - 1)])

    fields = pltpu.VMEM((FIELDS, plan.window_rows, columns), F32)
    return pl.pallas_call(
        functools.partial(main_kernel, plan),
        out_shape=[
            jax.ShapeDtypeStruct((PHASES, planes, rows, columns), F32),
            jax.ShapeDtypeStruct((SOLUTES, planes, rows, columns), F32),
        ],
        in_specs=[vmem, vmem, smem] + [vmem] * len(halos),
        out_specs=[hbm, hbm],
        scratch_shapes=[
            fields,
            fields,
            pltpu.VMEM((plan.window_rows, columns), F32),
            pltpu.VMEM((FIELDS, planes, rows, columns), F32),
            pltpu.SemaphoreType.DMA((2,)),
        ],
        name="steps",
    )(own, received, partition, *own_halos, *next_halos)


def solution(mesh):
    placed = (
        P("grow", "trans", None),
        P("grow", "trans", None),
        P(),
        P(),
        P(None, "grow", "trans", None),
        P(),
    )
    return jax.shard_map(
        shards,
        mesh=mesh,
        in_specs=placed,
        out_specs=(P(None, "grow", "trans", None), P(None, "grow", "trans", None)),
        check_vma=False,
    )
```

```python
import functools

import jax
import jax.numpy as jnp
from jax import lax
from jax.experimental import pallas as pl
from jax.experimental.pallas import tpu as pltpu
from jax.sharding import PartitionSpec as P


SHIFT = 16
STEPS = 3

PHASES = 4
SOLUTES = 2
FIELDS = PHASES + SOLUTES
RAW = 4

ANISOTROPY = 1.5
WELL_HEIGHT = 4.0
TIME_STEP = 0.06
LIQUID_DIFFUSION = 1.0
SOLID_DIFFUSION = 0.1
COOLING_WEIGHTS = (-1.0, 0.8, 0.7, 0.6)
FIRST_WEIGHTS = (0.5, -1.0, 0.4, 0.3)
SECOND_WEIGHTS = (0.4, 0.3, -1.0, 0.5)
INFLOW = (1.0, 0.0, 0.0, 0.0, 0.3, 0.2)
LIQUID_MOBILITY = 1.0

F32 = jnp.float32


class Plan:
    def __init__(self, planes, rows, slabs, blocks):
        self.planes, self.rows, self.slabs, self.blocks = planes, rows, slabs, blocks
        self.own = planes - SHIFT + STEPS
        self.next = SHIFT + STEPS
        self.depth = self.own + self.next
        self.pitch = (rows + 2 * STEPS) | 1
        self.window_rows = -(-self.depth * self.pitch // 8) * 8
        self.own_pieces, self.own_rows = self.pieces(0, self.own)
        self.next_pieces, self.next_rows = self.pieces(self.own, self.depth)

    def pieces(self, first, last):
        found, lengths = [], []
        for side in range(2):
            if self.blocks > 2 or not lengths:
                lengths.append(0)
            for j in range(first, last):
                for array in range(RAW):
                    inset = 1 if array == 3 else 0
                    count = min(STEPS - inset, j - inset, self.depth - 1 - inset - j)
                    if count > 0:
                        found.append((side, array, j, count, len(lengths) - 1, lengths[-1]))
                        lengths[-1] += count
        return found, [-(-length // 8) * 8 for length in lengths]


def pack_kernel(plan, phase, grain, solutes, orient, mobil, own, grow, *halos):
    rows = plan.rows
    table = jnp.zeros((rows, 128), F32)
    lanes = lax.broadcasted_iota(jnp.int32, (rows, 128), 1)
    for g in range(orient.shape[0]):
        table = jnp.where(lanes == g, mobil[orient[g]], table)
    own_halos = halos[: len(plan.own_rows)]
    next_halos = halos[len(plan.own_rows) :]
    first = SHIFT - STEPS
    where = {}
    for pieces, buffers, shift in ((plan.own_pieces, own_halos, first), (plan.next_pieces, next_halos, -plan.own)):
        for side, array, j, count, buffer, offset in pieces:
            where.setdefault((array, j + shift), []).append((side, count, buffers[buffer], offset))
    for z in range(plan.planes):
        label = phase[z].astype(F32)
        mobility = jnp.take_along_axis(table, grain[z], axis=1)
        for array, tile in enumerate((label, solutes[0, z], solutes[1, z], mobility)):
            if z >= first:
                own[array, z - first] = tile
            if z < plan.next:
                grow[array, z] = tile
            for side, count, buffer, offset in where.get((array, z), ()):
                piece = tile[:count] if side == 0 else tile[rows - count :]
                buffer[offset : offset + count, :] = piece


def step_tile(load, undercool, mobility, partition):
    centre = [load(f, 0, 0) for f in range(FIELDS)]
    below = [load(f, -1, 0) for f in range(FIELDS)]
    above = [load(f, 1, 0) for f in range(FIELDS)]
    prev = [load(f, 0, -1) for f in range(FIELDS)]
    after = [load(f, 0, 1) for f in range(FIELDS)]
    left = [pltpu.roll(c, 1, 1) for c in centre]
    right = [pltpu.roll(c, c.shape[1] - 1, 1) for c in centre]
    c0, c1 = centre[4], centre[5]
    forcing = []
    for a in range(PHASES):
        p = centre[a]
        laplace = ANISOTROPY * (above[a] + below[a]) + ((prev[a] + after[a]) + (left[a] + right[a]))
        laplace = laplace - (2.0 * ANISOTROPY + 4.0) * p
        driving = (COOLING_WEIGHTS[a] * undercool - 0.5) + FIRST_WEIGHTS[a] * c0 + SECOND_WEIGHTS[a] * c1
        well = WELL_HEIGHT * p
        forcing.append(laplace + (well - well * p) * (p + driving))
    mean = 0.25 * ((forcing[0] + forcing[1]) + (forcing[2] + forcing[3]))
    rate = TIME_STEP * mobility
    trials = [jnp.clip(centre[a] + rate * (forcing[a] - mean), 0.0, 1.0) for a in range(PHASES)]
    scale = 1.0 / ((trials[0] + trials[1]) + (trials[2] + trials[3]))
    phases = [t * scale for t in trials]
    slope = 0.5 * TIME_STEP * (LIQUID_DIFFUSION - SOLID_DIFFUSION)
    base = 0.5 * TIME_STEP * 2.0 * SOLID_DIFFUSION
    own = slope * centre[0] + base
    inflow = [None, None]
    for side in (above, below, prev, after, left, right):
        both = slope * side[0] + own
        for k in range(SOLUTES):
            flux = both * (side[4 + k] - centre[4 + k])
            inflow[k] = flux if inflow[k] is None else inflow[k] + flux
    changes = [phases[a] - centre[a] for a in range(PHASES)]
    solutes = []
    for k in range(SOLUTES):
        rejected = (partition[k, 0] * changes[0] + partition[k, 1] * changes[1]) + (
            partition[k, 2] * changes[2] + partition[k, 3] * changes[3]
        )
        solutes.append(centre[4 + k] + (inflow[k] - rejected))
    return phases + solutes


def main_kernel(plan, own, grow, partition, *refs):
    n_own, n_next = len(plan.own_rows), len(plan.next_rows)
    own_halos, next_halos = refs[:n_own], refs[n_own : n_own + n_next]
    phase_out, solute_out, field_a, field_b, mob, result, sems = refs[n_own + n_next :]
    rows, pitch, depth = plan.rows, plan.pitch, plan.depth
    slab = lax.axis_index("grow")
    first_slab, last_slab = slab == 0, slab == plan.slabs - 1
    edge = plan.own - 1
    total = plan.planes * plan.slabs

    def put(array, j, row, count, tile):
        spot = pl.ds(j * pitch + row, count)
        if array == 0:
            for a in range(PHASES):
                field_a[a, spot, :] = jnp.where(tile == a, 1.0, 0.0)
        elif array == 3:
            mob[spot, :] = tile
        else:
            field_a[PHASES - 1 + array, spot, :] = tile

    for j in range(depth):
        for array in range(RAW):
            tile = own[array, j] if j < plan.own else grow[array, j - plan.own]
            put(array, j, STEPS, rows, tile)
    for pieces, buffers in ((plan.own_pieces, own_halos), (plan.next_pieces, next_halos)):
        for side, array, j, count, buffer, offset in pieces:
            row = STEPS + rows if side == 0 else STEPS - count
            put(array, j, row, count, buffers[buffer][offset : offset + count, :])

    def repeat_edge(fields, source, target):
        for f in range(FIELDS):
            for row in (0, pitch - 8):
                fields[f, pl.ds(target * pitch + row, 8), :] = fields[f, pl.ds(source * pitch + row, 8), :]

    def sweep(source, target, begin, end, starts, base):
        def body(j, carry):
            height = (base + j).astype(F32)
            undercool = 2.0 * (0.5 - (height + 0.5) * (1.0 / total))
            for start in starts:
                at = j * pitch + start

                def load(f, dz, dr):
                    return source[f, pl.ds(at + dz * pitch + dr, 8), :]

                new = step_tile(load, undercool, mob[pl.ds(at, 8), :], partition)
                if target is None:
                    for f in range(FIELDS):
                        result[f, j - STEPS] = new[f]
                else:
                    for f in range(FIELDS):
                        target[f, pl.ds(at, 8), :] = new[f]
            return carry

        for j in range(begin, end):
            body(j, 0)

    origin = slab * plan.planes + SHIFT - STEPS

    @pl.when(last_slab)
    def _():
        repeat_edge(field_a, edge, edge + 1)

    sweep(field_a, field_b, 1, depth - 1, (1, rows + 2 * STEPS - 9), origin)

    @pl.when(last_slab)
    def _():
        repeat_edge(field_b, edge, edge + 1)

    sweep(field_b, field_a, 2, depth - 2, (2, rows + 2 * STEPS - 10), origin)

    @pl.when(last_slab)
    def _():
        for j in range(edge + 1, depth - 2):
            for row in (0, pitch - 8):
                spot = pl.ds(j * pitch + row, 8)
                for f in range(FIELDS):
                    field_a[f, spot, :] = jnp.full((8, 128), INFLOW[f], F32)
                mob[spot, :] = jnp.full((8, 128), LIQUID_MOBILITY, F32)

    @pl.when(first_slab)
    def _():
        repeat_edge(field_a, STEPS, STEPS - 1)

    sweep(field_a, None, STEPS, depth - STEPS, (STEPS,), slab * plan.planes - STEPS)
    copies = (
        pltpu.make_async_copy(result.at[pl.ds(0, PHASES)], phase_out, sems.at[0]),
        pltpu.make_async_copy(result.at[pl.ds(PHASES, SOLUTES)], solute_out, sems.at[1]),
    )
    for copy in copies:
        copy.start()
    for copy in copies:
        copy.wait()


def on_chip(value):
    return pltpu.with_memory_space_constraint(value, pltpu.VMEM)


def shards(phase_label, grain_label, grain_orient, orient_mobility, solute_init, partition):
    slabs, blocks = lax.axis_size("grow"), lax.axis_size("trans")
    planes, rows, columns = phase_label.shape
    plan = Plan(planes, rows, slabs, blocks)
    vmem, smem, hbm = (pl.BlockSpec(memory_space=m) for m in (pltpu.VMEM, pltpu.SMEM, pl.ANY))
    halo_shapes = [
        pltpu.VMEM((length, columns), F32) for length in plan.own_rows + plan.next_rows
    ]
    own, grow, *halos = pl.pallas_call(
        functools.partial(pack_kernel, plan),
        out_shape=[
            pltpu.VMEM((RAW, plan.own, rows, columns), F32),
            pltpu.VMEM((RAW, plan.next, rows, columns), F32),
            *halo_shapes,
        ],
        in_specs=[vmem, vmem, vmem, smem, smem],
        out_specs=[vmem] * (2 + len(halo_shapes)),
        name="pack",
    )(phase_label, grain_label, solute_init, grain_orient, orient_mobility)

    ups = [(b + 1) % blocks for b in range(blocks)]
    downs = [(b - 1) % blocks for b in range(blocks)]

    def fetch(value, side, hop):
        others = ups if side == 0 else downs
        pairs = [
            ((s + hop) * blocks + others[b], s * blocks + b) for s in range(slabs - hop) for b in range(blocks)
        ]
        return lax.ppermute(value, ("grow", "trans"), pairs)

    n_own = len(plan.own_rows)
    own_halos = [fetch(value, side, 0) for side, value in enumerate(halos[:n_own])]
    next_halos = [fetch(value, side, 1) for side, value in enumerate(halos[n_own:])]
    received = lax.ppermute(grow, "grow", [(s + 1, s) for s in range(slabs - 1)])

    fields = pltpu.VMEM((FIELDS, plan.window_rows, columns), F32)
    return pl.pallas_call(
        functools.partial(main_kernel, plan),
        out_shape=[
            jax.ShapeDtypeStruct((PHASES, planes, rows, columns), F32),
            jax.ShapeDtypeStruct((SOLUTES, planes, rows, columns), F32),
        ],
        in_specs=[vmem, vmem, smem] + [vmem] * len(halos),
        out_specs=[hbm, hbm],
        scratch_shapes=[
            fields,
            fields,
            pltpu.VMEM((plan.window_rows, columns), F32),
            pltpu.VMEM((FIELDS, planes, rows, columns), F32),
            pltpu.SemaphoreType.DMA((2,)),
        ],
        name="steps",
    )(*(on_chip(x) for x in (own, received)), partition.T, *(on_chip(x) for x in own_halos + next_halos))


def solution(mesh):
    placed = (
        P("grow", "trans", None),
        P("grow", "trans", None),
        P(),
        P(),
        P(None, "grow", "trans", None),
        P(),
    )
    return jax.shard_map(
        shards,
        mesh=mesh,
        in_specs=placed,
        out_specs=(P(None, "grow", "trans", None), P(None, "grow", "trans", None)),
        check_vma=False,
    )
```

```python
import functools

import jax
import jax.numpy as jnp
from jax import lax
from jax.experimental import pallas as pl
from jax.experimental.pallas import tpu as pltpu
from jax.sharding import PartitionSpec as P


SHIFT = 16
STEPS = 3

PHASES = 4
SOLUTES = 2
FIELDS = PHASES + SOLUTES
RAW = 4
TILE = 8

ANISOTROPY = 1.5
WELL_HEIGHT = 4.0
TIME_STEP = 0.06
LIQUID_DIFFUSION = 1.0
SOLID_DIFFUSION = 0.1
COOLING_WEIGHTS = (-1.0, 0.8, 0.7, 0.6)
FIRST_WEIGHTS = (0.5, -1.0, 0.4, 0.3)
SECOND_WEIGHTS = (0.4, 0.3, -1.0, 0.5)
INFLOW = (1.0, 0.0, 0.0, 0.0, 0.3, 0.2)
LIQUID_MOBILITY = 1.0

F32 = jnp.float32
PARAMS = pltpu.CompilerParams(vmem_limit_bytes=16 * 1024 * 1024)


def aligned(length):
    return -(-length // TILE) * TILE


class Plan:
    def __init__(self, planes, rows, slabs, blocks):
        self.planes, self.rows, self.slabs, self.blocks = planes, rows, slabs, blocks
        self.own = planes - SHIFT + STEPS
        self.next = SHIFT + STEPS
        self.depth = self.own + self.next
        self.wide = rows + 2 * STEPS
        self.pitch = aligned(self.depth + 2) + TILE
        self.total = planes * slabs
        self.own_runs, self.own_rows = self.runs(0, self.own)
        self.next_runs, self.next_rows = self.runs(self.own, self.depth)

    def runs(self, first, last):
        found, lengths = [], []
        for side in range(2):
            if self.blocks > 2 or not lengths:
                lengths.append(0)
            for array in range(RAW):
                inset = 1 if array == 3 else 0
                for distance in range(1, STEPS + 1 - inset):
                    low = max(first, distance + inset)
                    count = min(last, self.depth - distance - inset) - low
                    if count > 0:
                        found.append((side, array, distance, low, count, len(lengths) - 1, lengths[-1]))
                        lengths[-1] += count
        return found, [aligned(length) for length in lengths]

    def away(self, w):
        return max(0, STEPS - w, w - (STEPS + self.rows - 1))

    def starts(self, step, w):
        edge = step + self.away(w)
        low, high = edge, self.depth - edge
        return list(range(low, high - TILE, TILE)) + [high - TILE]


def pack_kernel(plan, *refs):
    inputs, (own, grow, rates, *halos), scratch = refs[:6], refs[6:-7], refs[-7:]
    *buffers, sems = scratch
    copies = [pltpu.make_async_copy(a, b, sems.at[i]) for i, (a, b) in enumerate(zip(inputs, buffers))]
    for copy in copies:
        copy.start()
    phase, grain, solutes, orient, mobil, partition = buffers
    for copy in copies[::-1]:
        copy.wait()
    rows = plan.rows
    for k in range(SOLUTES):
        for a in range(PHASES):
            rates[pl.ds((k * PHASES + a) * TILE, TILE), :] = jnp.full((TILE, 128), partition[k, a])
    table = jnp.zeros((rows, 128), F32)
    lanes = lax.broadcasted_iota(jnp.int32, (rows, 128), 1)
    for g in range(orient.shape[0]):
        table = jnp.where(lanes == g, mobil[orient[g]], table)
    first = SHIFT - STEPS
    for z in range(plan.planes):
        label = phase[z].astype(F32)
        mobility = jnp.take_along_axis(table, grain[z], axis=1)
        for array, tile in enumerate((label, solutes[0, z], solutes[1, z], mobility)):
            if z >= first:
                own[pl.ds((array * plan.own + z - first) * rows, rows), :] = tile
            if z < plan.next:
                grow[pl.ds((array * plan.next + z) * rows, rows), :] = tile
    n_own = len(plan.own_rows)
    for source, begin, length, runs, buffers in (
        (grow, plan.own, plan.next, plan.next_runs, halos[n_own:]),
        (own, 0, plan.own, plan.own_runs, halos[:n_own]),
    ):
        for side, array, distance, j, count, buffer, offset in runs:
            row = distance - 1 if side == 0 else rows - distance
            for k in range(0, count, TILE):
                n = min(TILE, count - k)
                at = (array * length + j - begin + k) * rows + row
                buffers[buffer][pl.ds(offset + k, n), :] = source[pl.ds(at, n, stride=rows), :]


def step_tile(load, cooling, mobility, partition):
    centre = [load(f, 0, 0) for f in range(FIELDS)]
    below = [load(f, -1, 0) for f in range(FIELDS)]
    above = [load(f, 1, 0) for f in range(FIELDS)]
    prev = [load(f, 0, -1) for f in range(FIELDS)]
    after = [load(f, 0, 1) for f in range(FIELDS)]
    left = [pltpu.roll(c, 1, 1) for c in centre]
    right = [pltpu.roll(c, c.shape[1] - 1, 1) for c in centre]
    c0, c1 = centre[4], centre[5]
    forcing = []
    for a in range(PHASES):
        p = centre[a]
        laplace = ANISOTROPY * (above[a] + below[a]) + ((prev[a] + after[a]) + (left[a] + right[a]))
        laplace = laplace - (2.0 * ANISOTROPY + 4.0) * p
        driving = cooling(a) + FIRST_WEIGHTS[a] * c0 + SECOND_WEIGHTS[a] * c1
        well = WELL_HEIGHT * p
        forcing.append(laplace + (well - well * p) * (p + driving))
    mean = 0.25 * ((forcing[0] + forcing[1]) + (forcing[2] + forcing[3]))
    rate = TIME_STEP * mobility
    trials = [jnp.clip(centre[a] + rate * (forcing[a] - mean), 0.0, 1.0) for a in range(PHASES)]
    scale = 1.0 / ((trials[0] + trials[1]) + (trials[2] + trials[3]))
    phases = [t * scale for t in trials]
    slope = 0.5 * TIME_STEP * (LIQUID_DIFFUSION - SOLID_DIFFUSION)
    base = 0.5 * TIME_STEP * 2.0 * SOLID_DIFFUSION
    own = slope * centre[0] + base
    inflow = [None, None]
    for side in (above, below, prev, after, left, right):
        both = slope * side[0] + own
        for k in range(SOLUTES):
            flux = both * (side[4 + k] - centre[4 + k])
            inflow[k] = flux if inflow[k] is None else inflow[k] + flux
    changes = [phases[a] - centre[a] for a in range(PHASES)]
    solutes = []
    for k in range(SOLUTES):
        rejected = (partition(k, 0) * changes[0] + partition(k, 1) * changes[1]) + (
            partition(k, 2) * changes[2] + partition(k, 3) * changes[3]
        )
        solutes.append(centre[4 + k] + (inflow[k] - rejected))
    return phases + solutes


class Rows:
    def __init__(self, plan, *groups):
        self.pitch = plan.pitch
        self.place = {}
        for ref, rows in groups:
            for slot, w in enumerate(rows):
                self.place[w] = (ref, slot * plan.pitch)

    def load(self, f, w, j, count=TILE):
        ref, base = self.place[w]
        return ref[f, pl.ds(base + j, count), :]

    def store(self, f, w, j, value):
        ref, base = self.place[w]
        ref[f, pl.ds(base + j, value.shape[0]), :] = value


def fill_cooling(plan, cooling, first):
    ramp = lax.broadcasted_iota(jnp.int32, (TILE, 128), 0)
    for j in range(0, plan.depth, TILE):
        height = (ramp + (first + j)).astype(F32)
        undercool = 2.0 * (0.5 - (height + 0.5) * (1.0 / plan.total))
        for a in range(PHASES):
            cooling[a, pl.ds(j, TILE), :] = COOLING_WEIGHTS[a] * undercool - 0.5


def sweep(w, j, source, mobility, cooling, partition):
    def load(f, dz, dr):
        return source.load(f, w + dr, j + dz)

    def rate(k, a):
        return partition[pl.ds((k * PHASES + a) * TILE, TILE), :]

    return step_tile(load, lambda a: cooling[a, pl.ds(j, TILE), :], mobility.load(0, w, j), rate)


def run_step(plan, step, rows, source, target, mobility, cooling, partition):
    for w in rows:
        for j in plan.starts(step, w):
            new = sweep(w, j, source, mobility, cooling, partition)
            for f in range(FIELDS):
                target.store(f, w, j, new[f])


def repeat_plane(fields, rows, source, target):
    for w in rows:
        for f in range(FIELDS):
            fields.store(f, w, target, fields.load(f, w, source, 1))


def fill_liquid(plan, fields, rows):
    count = plan.depth - 2 - plan.own
    for w in rows:
        for f in range(FIELDS):
            fields.store(f, w, plan.own, jnp.full((count, 128), INFLOW[f], F32))


def put_raw(fields, mobility, array, w, j, tile):
    if array == 0:
        for a in range(PHASES):
            fields.store(a, w, j, jnp.where(tile == a, 1.0, 0.0))
    elif array == 3:
        mobility.store(0, w, j, tile)
    else:
        fields.store(PHASES - 1 + array, w, j, tile)


def row_sets(plan):
    own = list(range(STEPS, STEPS + plan.rows))
    inner = [own[step:-step] for step in range(STEPS + 1)]
    outer = [
        [w for w in range(step, plan.wide - step) if w not in inner[step]] for step in range(STEPS + 1)
    ]
    inner[0] = own
    outer[0] = [w for w in range(plan.wide) if w not in own]
    return inner, outer


def inner_kernel(plan, own, grow, partition, f0, m0, f1, f2, f3, cooling, late_cooling):
    rows = plan.rows
    inner, _ = row_sets(plan)
    slab = lax.axis_index("grow")
    first_slab, last_slab = slab == 0, slab == plan.slabs - 1
    edge = plan.own - 1
    raw, mobility = Rows(plan, (f0, inner[0])), Rows(plan, (m0, inner[0]))
    once, twice, final = Rows(plan, (f1, inner[1])), Rows(plan, (f2, inner[2])), Rows(plan, (f3, inner[3]))
    fill_cooling(plan, cooling, slab * plan.planes + SHIFT - STEPS)
    fill_cooling(plan, late_cooling, slab * plan.planes - STEPS)

    for array in range(RAW):
        for source, begin, length in ((own, 0, plan.own), (grow, plan.own, plan.next)):
            for w in inner[0]:
                for k in range(0, length, TILE):
                    n = min(TILE, length - k)
                    at = (array * length + k) * rows + w - STEPS
                    put_raw(raw, mobility, array, w, begin + k, source[pl.ds(at, n, stride=rows), :])

    @pl.when(last_slab)
    def _():
        repeat_plane(raw, inner[0], edge, edge + 1)

    run_step(plan, 1, inner[1], raw, once, mobility, cooling, partition)

    @pl.when(last_slab)
    def _():
        repeat_plane(once, inner[1], edge, edge + 1)

    run_step(plan, 2, inner[2], once, twice, mobility, cooling, partition)

    @pl.when(last_slab)
    def _():
        fill_liquid(plan, twice, inner[2])
        count = plan.depth - 2 - plan.own
        for w in inner[0]:
            mobility.store(0, w, plan.own, jnp.full((count, 128), LIQUID_MOBILITY, F32))

    @pl.when(first_slab)
    def _():
        repeat_plane(twice, inner[2], STEPS, STEPS - 1)

    run_step(plan, 3, inner[3], twice, final, mobility, late_cooling, partition)


def outer_kernel(plan, f0, m0, f1, f2, f3, partition, *refs):
    n_own, n_next = len(plan.own_rows), len(plan.next_rows)
    own_halos, next_halos = refs[:n_own], refs[n_own : n_own + 2 * n_next]
    phase_out, solute_out, x0, xm, x1, x2, result, cooling, late_cooling, sems = refs[n_own + 2 * n_next :]
    rows = plan.rows
    inner, outer = row_sets(plan)
    slab = lax.axis_index("grow")
    first_slab, last_slab = slab == 0, slab == plan.slabs - 1
    odd = lax.rem(slab, 2) == 1
    edge = plan.own - 1
    raw = Rows(plan, (f0, inner[0]), (x0, outer[0]))
    mobility = Rows(plan, (m0, inner[0]), (xm, [w for w in outer[0] if plan.away(w) < STEPS]))
    once, twice = Rows(plan, (f1, inner[1]), (x1, outer[1])), Rows(plan, (f2, inner[2]), (x2, outer[2]))
    done = Rows(plan, (f3, inner[3]))
    fill_cooling(plan, cooling, slab * plan.planes + SHIFT - STEPS)
    fill_cooling(plan, late_cooling, slab * plan.planes - STEPS)

    for runs, buffers in ((plan.own_runs, own_halos), (plan.next_runs, next_halos)):
        for side, array, distance, j, count, buffer, offset in runs:
            w = STEPS + rows - 1 + distance if side == 0 else STEPS - distance
            for k in range(0, count, TILE):
                n = min(TILE, count - k)
                tile = buffers[buffer][pl.ds(offset + k, n), :]
                if len(buffers) > n_next:
                    tile = jnp.where(odd, buffers[buffer + n_next][pl.ds(offset + k, n), :], tile)
                put_raw(raw, mobility, array, w, j + k, tile)

    @pl.when(last_slab)
    def _():
        repeat_plane(raw, outer[0], edge, edge + 1)

    run_step(plan, 1, outer[1], raw, once, mobility, cooling, partition)

    @pl.when(last_slab)
    def _():
        repeat_plane(once, outer[1], edge, edge + 1)

    run_step(plan, 2, outer[2], once, twice, mobility, cooling, partition)

    @pl.when(last_slab)
    def _():
        fill_liquid(plan, twice, outer[2])

    @pl.when(first_slab)
    def _():
        repeat_plane(twice, outer[2], STEPS, STEPS - 1)

    copies = []
    sent = 0
    for j in plan.starts(3, STEPS):
        for w in inner[0]:
            if w in inner[3]:
                new = [done.load(f, w, j) for f in range(FIELDS)]
            else:
                new = sweep(w, j, twice, mobility, late_cooling, partition)
            for f in range(FIELDS):
                result[f, pl.ds((j - STEPS) * rows + w - STEPS, TILE, stride=rows), :] = new[f]
        ready = (j - STEPS + TILE) * rows
        part = pl.ds(sent, ready - sent)
        for out, begin, count in ((phase_out, 0, PHASES), (solute_out, PHASES, SOLUTES)):
            copies.append(
                pltpu.make_async_copy(
                    result.at[pl.ds(begin, count), part], out.at[:, part], sems.at[len(copies)]
                )
            )
            copies[-1].start()
        sent = ready
    for copy in copies:
        copy.wait()


def on_chip(value):
    return pltpu.with_memory_space_constraint(value, pltpu.VMEM)


def shards(phase_label, grain_label, grain_orient, orient_mobility, solute_init, partition):
    slabs, blocks = lax.axis_size("grow"), lax.axis_size("trans")
    planes, rows, columns = phase_label.shape
    plan = Plan(planes, rows, slabs, blocks)
    inner, outer = row_sets(plan)
    vmem, hbm = (pl.BlockSpec(memory_space=m) for m in (pltpu.VMEM, pltpu.HBM))

    def field_rows(count, fields=FIELDS):
        return pltpu.VMEM((fields, count * plan.pitch, columns), F32)

    halo_shapes = [pltpu.VMEM((length, columns), F32) for length in plan.own_rows + plan.next_rows]
    inputs = (phase_label, grain_label, solute_init, grain_orient, orient_mobility, partition.T)
    own, grow, rates, *halos = pl.pallas_call(
        functools.partial(pack_kernel, plan),
        out_shape=[
            pltpu.VMEM((RAW * plan.own * rows, columns), F32),
            pltpu.VMEM((RAW * plan.next * rows, columns), F32),
            pltpu.VMEM((SOLUTES * PHASES * TILE, columns), F32),
            *halo_shapes,
        ],
        in_specs=[hbm] * len(inputs),
        out_specs=[vmem] * (3 + len(halo_shapes)),
        scratch_shapes=[
            (pltpu.VMEM if value.ndim > 2 else pltpu.SMEM)(value.shape, value.dtype) for value in inputs
        ]
        + [pltpu.SemaphoreType.DMA((len(inputs),))],
        compiler_params=PARAMS,
        name="pack",
    )(*(pltpu.with_memory_space_constraint(value, pltpu.HBM) for value in inputs))

    ups = [(b + 1) % blocks for b in range(blocks)]
    downs = [(b - 1) % blocks for b in range(blocks)]

    def fetch(value, side, hop, targets, closed=True):
        others = ups if side == 0 else downs
        pairs = [(((s + hop) % slabs) * blocks + others[b], s * blocks + b) for s in targets for b in range(blocks)]
        if closed:
            senders, takers = ({pair[i] for pair in pairs} for i in range(2))
            idle = [
                [i for i in range(slabs * blocks) if i not in busy] for busy in (senders, takers)
            ]
            pairs += zip(*(sorted(i, key=lambda d: (d // blocks // 2, d % blocks)) for i in idle))
        return lax.ppermute(value, ("grow", "trans"), pairs)

    n_own = len(plan.own_rows)
    own_halos = [fetch(value, side, 0, range(slabs)) for side, value in enumerate(halos[:n_own])]
    even_halos = [fetch(v, side, 1, range(0, slabs - 1, 2)) for side, v in enumerate(halos[n_own:])]
    odd_halos = [fetch(v, side, 1, range(1, slabs - 1, 2), closed=False) for side, v in enumerate(halos[n_own:])]
    received = lax.ppermute(grow, "grow", [(s + 1, s) for s in range(slabs - 1)])
    cooling = pltpu.VMEM((PHASES, plan.pitch, columns), F32)
    state = pl.pallas_call(
        functools.partial(inner_kernel, plan),
        out_shape=[
            field_rows(len(inner[0])),
            field_rows(len(inner[0]), 1),
            field_rows(len(inner[1])),
            field_rows(len(inner[2])),
            field_rows(len(inner[3])),
        ],
        in_specs=[vmem] * 3,
        out_specs=[vmem] * 5,
        scratch_shapes=[cooling, cooling],
        cost_estimate=pl.CostEstimate(flops=8_000_000, bytes_accessed=0, transcendentals=0),
        compiler_params=PARAMS,
        name="inner",
    )(*(on_chip(x) for x in (own, received, rates)))
    halos = own_halos + even_halos + odd_halos
    phase_out, solute_out = pl.pallas_call(
        functools.partial(outer_kernel, plan),
        out_shape=[
            jax.ShapeDtypeStruct((PHASES, planes * rows, columns), F32),
            jax.ShapeDtypeStruct((SOLUTES, planes * rows, columns), F32),
        ],
        in_specs=[vmem] * (6 + len(halos)),
        out_specs=[hbm, hbm],
        scratch_shapes=[
            field_rows(len(outer[0])),
            field_rows(len(outer[0]) - 2, 1),
            field_rows(len(outer[1])),
            field_rows(len(outer[2])),
            pltpu.VMEM((FIELDS, planes * rows, columns), F32),
            cooling,
            cooling,
            pltpu.SemaphoreType.DMA((2 * len(plan.starts(3, STEPS)),)),
        ],
        cost_estimate=pl.CostEstimate(flops=8_000_000, bytes_accessed=0, transcendentals=0),
        compiler_params=PARAMS,
        name="outer",
    )(*(on_chip(x) for x in (*state, rates, *halos)))
    return (
        phase_out.reshape(PHASES, planes, rows, columns),
        solute_out.reshape(SOLUTES, planes, rows, columns),
    )


def solution(mesh):
    placed = (
        P("grow", "trans", None),
        P("grow", "trans", None),
        P(),
        P(),
        P(None, "grow", "trans", None),
        P(),
    )
    return jax.shard_map(
        shards,
        mesh=mesh,
        in_specs=placed,
        out_specs=(P(None, "grow", "trans", None), P(None, "grow", "trans", None)),
        check_vma=False,
    )
```

```python
import functools

import jax
import jax.numpy as jnp
from jax import lax
from jax.experimental import pallas as pl
from jax.experimental.pallas import tpu as pltpu
from jax.sharding import PartitionSpec as P


SHIFT = 16
STEPS = 3

PHASES = 4
SOLUTES = 2
FIELDS = PHASES + SOLUTES
STORED = FIELDS + SOLUTES
RAW = 4
TILE = 8

ANISOTROPY = 1.5
WELL_HEIGHT = 4.0
TIME_STEP = 0.06
LIQUID_DIFFUSION = 1.0
SOLID_DIFFUSION = 0.1
COOLING_WEIGHTS = (-1.0, 0.8, 0.7, 0.6)
FIRST_WEIGHTS = (0.5, -1.0, 0.4, 0.3)
SECOND_WEIGHTS = (0.4, 0.3, -1.0, 0.5)
INFLOW = (1.0, 0.0, 0.0, 0.0, 0.3, 0.2)
LIQUID_MOBILITY = 1.0
SLOPE = 0.5 * TIME_STEP * (LIQUID_DIFFUSION - SOLID_DIFFUSION)
BASE = 0.5 * TIME_STEP * 2.0 * SOLID_DIFFUSION
INFLOW = INFLOW + (SLOPE * INFLOW[0] * INFLOW[4], SLOPE * INFLOW[0] * INFLOW[5])

F32 = jnp.float32
PARAMS = pltpu.CompilerParams(vmem_limit_bytes=16 * 1024 * 1024)


def aligned(length):
    return -(-length // TILE) * TILE


class Plan:
    def __init__(self, planes, rows, columns, slabs, blocks):
        self.planes, self.rows, self.columns, self.slabs, self.blocks = planes, rows, columns, slabs, blocks
        self.own = planes - SHIFT + STEPS
        self.next = SHIFT + STEPS
        self.depth = self.own + self.next
        self.wide = rows + 2 * STEPS
        self.pitch = aligned(self.depth + 2) + TILE
        self.total = planes * slabs
        self.own_runs, self.own_rows = self.runs(0, self.own)
        self.next_runs, self.next_rows = self.runs(self.own, self.depth)

    def runs(self, first, last):
        found, lengths = [], []
        for side in range(2):
            if self.blocks > 2 or not lengths:
                lengths.append(0)
            for array in range(RAW):
                inset = 1 if array == 3 else 0
                for distance in range(1, STEPS + 1 - inset):
                    low = max(first, distance + inset)
                    count = min(last, self.depth - distance - inset) - low
                    if count > 0:
                        found.append((side, array, distance, low, count, len(lengths) - 1, lengths[-1]))
                        lengths[-1] += count
        return found, [aligned(length) for length in lengths]

    def away(self, w):
        return max(0, STEPS - w, w - (STEPS + self.rows - 1))

    def starts(self, step, w):
        edge = step + self.away(w)
        low, high = edge, self.depth - edge
        return list(range(low, high - TILE, TILE)) + [high - TILE]


def pack_kernel(plan, *refs):
    inputs, (own, grow, rates, *halos), scratch = refs[:6], refs[6:-7], refs[-7:]
    *buffers, sems = scratch
    copies = [pltpu.make_async_copy(a, b, sems.at[i]) for i, (a, b) in enumerate(zip(inputs, buffers))]
    for copy in copies:
        copy.start()
    phase, grain, solutes, orient, mobil, partition = buffers
    for copy in copies[::-1]:
        copy.wait()
    rows = plan.rows
    for k in range(SOLUTES):
        for a in range(PHASES):
            rates[pl.ds((k * PHASES + a) * TILE, TILE), :] = jnp.full((TILE, plan.columns), partition[k, a])
    table = jnp.zeros((rows, plan.columns), F32)
    lanes = lax.broadcasted_iota(jnp.int32, (rows, plan.columns), 1)
    for g in range(orient.shape[0]):
        table = jnp.where(lanes == g, TIME_STEP * mobil[orient[g]], table)
    first = SHIFT - STEPS
    for z in range(plan.planes):
        label = phase[z].astype(F32)
        mobility = jnp.take_along_axis(table, grain[z], axis=1)
        for array, tile in enumerate((label, solutes[0, z], solutes[1, z], mobility)):
            if z >= first:
                own[pl.ds((array * plan.own + z - first) * rows, rows), :] = tile
            if z < plan.next:
                grow[pl.ds((array * plan.next + z) * rows, rows), :] = tile
    n_own = len(plan.own_rows)
    for source, begin, length, runs, buffers in (
        (grow, plan.own, plan.next, plan.next_runs, halos[n_own:]),
        (own, 0, plan.own, plan.own_runs, halos[:n_own]),
    ):
        for side, array, distance, j, count, buffer, offset in runs:
            row = distance - 1 if side == 0 else rows - distance
            for k in range(0, count, TILE):
                n = min(TILE, count - k)
                at = (array * length + j - begin + k) * rows + row
                buffers[buffer][pl.ds(offset + k, n), :] = source[pl.ds(at, n, stride=rows), :]


def step_tile(load, cooling, rate, partition):
    centre = [load(f, 0, 0) for f in range(STORED)]
    depth, flat = [], []
    for f in range(STORED):
        depth.append(load(f, 1, 0) + load(f, -1, 0))
        turned = pltpu.roll(centre[f], 1, 1) + pltpu.roll(centre[f], centre[f].shape[1] - 1, 1)
        flat.append((load(f, 0, -1) + load(f, 0, 1)) + turned)
    c0, c1 = centre[4], centre[5]
    forcing = []
    for a in range(PHASES):
        p = centre[a]
        driving = cooling(a) + (WELL_HEIGHT * FIRST_WEIGHTS[a]) * c0 + (WELL_HEIGHT * SECOND_WEIGHTS[a]) * c1
        well = (1.0 - p) * (WELL_HEIGHT * p + driving) - (2.0 * ANISOTROPY + 4.0)
        forcing.append((ANISOTROPY * depth[a] + flat[a]) + p * well)
    mean = 0.25 * ((forcing[0] + forcing[1]) + (forcing[2] + forcing[3]))
    trials = [jnp.clip(centre[a] + rate * (forcing[a] - mean), 0.0, 1.0) for a in range(PHASES)]
    scale = 1.0 / ((trials[0] + trials[1]) + (trials[2] + trials[3]))
    phases = [t * scale for t in trials]
    own = SLOPE * centre[0] + BASE
    outflow = SLOPE * (depth[0] + flat[0]) + 6.0 * own
    changes = [phases[a] - centre[a] for a in range(PHASES)]
    solutes = []
    for k in range(SOLUTES):
        c, product = 4 + k, FIELDS + k
        inflow = (depth[product] + flat[product]) + own * (depth[c] + flat[c]) - outflow * centre[c]
        rejected = (partition(k, 0) * changes[0] + partition(k, 1) * changes[1]) + (
            partition(k, 2) * changes[2] + partition(k, 3) * changes[3]
        )
        solutes.append(centre[c] + (inflow - rejected))
    return phases + solutes


class Rows:
    def __init__(self, plan, *groups):
        self.pitch = plan.pitch
        self.place = {}
        for ref, rows in groups:
            for slot, w in enumerate(rows):
                self.place[w] = (ref, slot * plan.pitch)

    def load(self, f, w, j, count=TILE):
        ref, base = self.place[w]
        return ref[f, pl.ds(base + j, count), :]

    def store(self, f, w, j, value):
        ref, base = self.place[w]
        ref[f, pl.ds(base + j, value.shape[0]), :] = value


def fill_cooling(plan, cooling, first):
    ramp = lax.broadcasted_iota(jnp.int32, (TILE, plan.columns), 0)
    for j in range(0, plan.depth, TILE):
        height = (ramp + (first + j)).astype(F32)
        undercool = 2.0 * (0.5 - (height + 0.5) * (1.0 / plan.total))
        for a in range(PHASES):
            cooling[a, pl.ds(j, TILE), :] = WELL_HEIGHT * (COOLING_WEIGHTS[a] * undercool - 0.5)


def sweep(w, j, source, mobility, cooling, partition):
    def load(f, dz, dr):
        return source.load(f, w + dr, j + dz)

    def rate(k, a):
        return partition[pl.ds((k * PHASES + a) * TILE, TILE), :]

    return step_tile(load, lambda a: cooling[a, pl.ds(j, TILE), :], mobility.load(0, w, j), rate)


def run_step(plan, step, rows, source, target, mobility, cooling, partition):
    for w in rows:
        for j in plan.starts(step, w):
            new = sweep(w, j, source, mobility, cooling, partition)
            liquid = SLOPE * new[0]
            for f, value in enumerate(new + [liquid * c for c in new[PHASES:]]):
                target.store(f, w, j, value)


def repeat_plane(fields, rows, source, target):
    for w in rows:
        for f in range(STORED):
            fields.store(f, w, target, fields.load(f, w, source, 1))


def fill_liquid(plan, fields, rows):
    count = plan.depth - 2 - plan.own
    for w in rows:
        for f in range(STORED):
            fields.store(f, w, plan.own, jnp.full((count, plan.columns), INFLOW[f], F32))


def put_raw(fields, mobility, array, w, j, tile):
    if array == 0:
        for a in range(PHASES):
            fields.store(a, w, j, jnp.where(tile == a, 1.0, 0.0))
    elif array == 3:
        mobility.store(0, w, j, tile)
    else:
        fields.store(PHASES - 1 + array, w, j, tile)
        fields.store(FIELDS - 1 + array, w, j, SLOPE * fields.load(0, w, j, tile.shape[0]) * tile)


def row_sets(plan):
    own = list(range(STEPS, STEPS + plan.rows))
    inner = [own[step:-step] for step in range(STEPS + 1)]
    outer = [
        [w for w in range(step, plan.wide - step) if w not in inner[step]] for step in range(STEPS + 1)
    ]
    inner[0] = own
    outer[0] = [w for w in range(plan.wide) if w not in own]
    return inner, outer


def inner_kernel(plan, own, grow, partition, f0, m0, f1, f2, f3, cooling, late_cooling):
    rows = plan.rows
    inner, _ = row_sets(plan)
    slab = lax.axis_index("grow")
    first_slab, last_slab = slab == 0, slab == plan.slabs - 1
    edge = plan.own - 1
    raw, mobility = Rows(plan, (f0, inner[0])), Rows(plan, (m0, inner[0]))
    once, twice, final = Rows(plan, (f1, inner[1])), Rows(plan, (f2, inner[2])), Rows(plan, (f3, inner[3]))
    fill_cooling(plan, cooling, slab * plan.planes + SHIFT - STEPS)
    fill_cooling(plan, late_cooling, slab * plan.planes - STEPS)

    for array in range(RAW):
        for source, begin, length in ((own, 0, plan.own), (grow, plan.own, plan.next)):
            for w in inner[0]:
                for k in range(0, length, TILE):
                    n = min(TILE, length - k)
                    at = (array * length + k) * rows + w - STEPS
                    put_raw(raw, mobility, array, w, begin + k, source[pl.ds(at, n, stride=rows), :])

    @pl.when(last_slab)
    def _():
        repeat_plane(raw, inner[0], edge, edge + 1)

    run_step(plan, 1, inner[1], raw, once, mobility, cooling, partition)

    @pl.when(last_slab)
    def _():
        repeat_plane(once, inner[1], edge, edge + 1)

    run_step(plan, 2, inner[2], once, twice, mobility, cooling, partition)

    @pl.when(last_slab)
    def _():
        fill_liquid(plan, twice, inner[2])
        count = plan.depth - 2 - plan.own
        for w in inner[0]:
            mobility.store(0, w, plan.own, jnp.full((count, plan.columns), TIME_STEP * LIQUID_MOBILITY, F32))

    @pl.when(first_slab)
    def _():
        repeat_plane(twice, inner[2], STEPS, STEPS - 1)

    for w in inner[3]:
        for j in plan.starts(3, w):
            new = sweep(w, j, twice, mobility, late_cooling, partition)
            for f in range(FIELDS):
                final.store(f, w, j, new[f])


def outer_kernel(plan, f0, m0, f1, f2, f3, partition, *refs):
    n_own, n_next = len(plan.own_rows), len(plan.next_rows)
    own_halos, next_halos = refs[:n_own], refs[n_own : n_own + 2 * n_next]
    phase_out, solute_out, x0, xm, x1, x2, result, cooling, late_cooling, sems = refs[n_own + 2 * n_next :]
    rows = plan.rows
    inner, outer = row_sets(plan)
    slab = lax.axis_index("grow")
    first_slab, last_slab = slab == 0, slab == plan.slabs - 1
    odd = lax.rem(slab, 2) == 1
    edge = plan.own - 1
    raw = Rows(plan, (f0, inner[0]), (x0, outer[0]))
    mobility = Rows(plan, (m0, inner[0]), (xm, [w for w in outer[0] if plan.away(w) < STEPS]))
    once, twice = Rows(plan, (f1, inner[1]), (x1, outer[1])), Rows(plan, (f2, inner[2]), (x2, outer[2]))
    done = Rows(plan, (f3, inner[3]))
    fill_cooling(plan, cooling, slab * plan.planes + SHIFT - STEPS)
    fill_cooling(plan, late_cooling, slab * plan.planes - STEPS)

    for runs, buffers in ((plan.own_runs, own_halos), (plan.next_runs, next_halos)):
        for side, array, distance, j, count, buffer, offset in runs:
            w = STEPS + rows - 1 + distance if side == 0 else STEPS - distance
            for k in range(0, count, TILE):
                n = min(TILE, count - k)
                tile = buffers[buffer][pl.ds(offset + k, n), :]
                if len(buffers) > n_next:
                    tile = jnp.where(odd, buffers[buffer + n_next][pl.ds(offset + k, n), :], tile)
                put_raw(raw, mobility, array, w, j + k, tile)

    @pl.when(last_slab)
    def _():
        repeat_plane(raw, outer[0], edge, edge + 1)

    run_step(plan, 1, outer[1], raw, once, mobility, cooling, partition)

    @pl.when(last_slab)
    def _():
        repeat_plane(once, outer[1], edge, edge + 1)

    run_step(plan, 2, outer[2], once, twice, mobility, cooling, partition)

    @pl.when(last_slab)
    def _():
        fill_liquid(plan, twice, outer[2])

    @pl.when(first_slab)
    def _():
        repeat_plane(twice, outer[2], STEPS, STEPS - 1)

    copies = []
    sent = 0
    for j in plan.starts(3, STEPS):
        for w in inner[0]:
            if w in inner[3]:
                new = [done.load(f, w, j) for f in range(FIELDS)]
            else:
                new = sweep(w, j, twice, mobility, late_cooling, partition)
            for f in range(FIELDS):
                result[f, pl.ds((j - STEPS) * rows + w - STEPS, TILE, stride=rows), :] = new[f]
        ready = (j - STEPS + TILE) * rows
        part = pl.ds(sent, ready - sent)
        for out, begin, count in ((phase_out, 0, PHASES), (solute_out, PHASES, SOLUTES)):
            copies.append(
                pltpu.make_async_copy(
                    result.at[pl.ds(begin, count), part], out.at[:, part], sems.at[len(copies)]
                )
            )
            copies[-1].start()
        sent = ready
    for copy in copies:
        copy.wait()


def on_chip(value):
    return pltpu.with_memory_space_constraint(value, pltpu.VMEM)


def shards(phase_label, grain_label, grain_orient, orient_mobility, solute_init, partition):
    slabs, blocks = lax.axis_size("grow"), lax.axis_size("trans")
    planes, rows, columns = phase_label.shape
    plan = Plan(planes, rows, columns, slabs, blocks)
    inner, outer = row_sets(plan)
    vmem, hbm = (pl.BlockSpec(memory_space=m) for m in (pltpu.VMEM, pltpu.HBM))

    def field_rows(count, fields=STORED):
        return pltpu.VMEM((fields, count * plan.pitch, columns), F32)

    halo_shapes = [pltpu.VMEM((length, columns), F32) for length in plan.own_rows + plan.next_rows]
    inputs = (phase_label, grain_label, solute_init, grain_orient, orient_mobility, partition.T)
    own, grow, rates, *halos = pl.pallas_call(
        functools.partial(pack_kernel, plan),
        out_shape=[
            pltpu.VMEM((RAW * plan.own * rows, columns), F32),
            pltpu.VMEM((RAW * plan.next * rows, columns), F32),
            pltpu.VMEM((SOLUTES * PHASES * TILE, columns), F32),
            *halo_shapes,
        ],
        in_specs=[hbm] * len(inputs),
        out_specs=[vmem] * (3 + len(halo_shapes)),
        scratch_shapes=[
            (pltpu.VMEM if value.ndim > 2 else pltpu.SMEM)(value.shape, value.dtype) for value in inputs
        ]
        + [pltpu.SemaphoreType.DMA((len(inputs),))],
        compiler_params=PARAMS,
        name="pack",
    )(*(pltpu.with_memory_space_constraint(value, pltpu.HBM) for value in inputs))

    ups = [(b + 1) % blocks for b in range(blocks)]
    downs = [(b - 1) % blocks for b in range(blocks)]

    def fetch(value, side, hop, targets, closed=True):
        others = ups if side == 0 else downs
        pairs = [
            ((s + hop) * blocks + others[b] if s + hop < slabs else b, s * blocks + b)
            for s in targets
            for b in range(blocks)
        ]
        if closed:
            senders, takers = ({pair[i] for pair in pairs} for i in range(2))
            idle = [
                [i for i in range(slabs * blocks) if i not in busy] for busy in (senders, takers)
            ]
            pairs += zip(*(sorted(i, key=lambda d: (d // blocks // 2, d % blocks)) for i in idle))
        return lax.ppermute(value, ("grow", "trans"), pairs)

    n_own = len(plan.own_rows)
    own_halos = [fetch(value, side, 0, range(slabs)) for side, value in enumerate(halos[:n_own])]
    even_halos = [fetch(v, side, 1, range(0, slabs - 1, 2)) for side, v in enumerate(halos[n_own:])]
    odd_halos = [fetch(v, side, 1, range(1, slabs, 2)) for side, v in enumerate(halos[n_own:])]
    received = lax.ppermute(grow, "grow", [(s + 1, s) for s in range(slabs - 1)])
    cooling = pltpu.VMEM((PHASES, plan.pitch, columns), F32)
    state = pl.pallas_call(
        functools.partial(inner_kernel, plan),
        out_shape=[
            field_rows(len(inner[0])),
            field_rows(len(inner[0]), 1),
            field_rows(len(inner[1])),
            field_rows(len(inner[2])),
            field_rows(len(inner[3]), FIELDS),
        ],
        in_specs=[vmem] * 3,
        out_specs=[vmem] * 5,
        scratch_shapes=[cooling, cooling],
        cost_estimate=pl.CostEstimate(flops=8_000_000, bytes_accessed=0, transcendentals=0),
        compiler_params=PARAMS,
        name="inner",
    )(*(on_chip(x) for x in (own, received, rates)))
    halos = own_halos + even_halos + odd_halos
    phase_out, solute_out = pl.pallas_call(
        functools.partial(outer_kernel, plan),
        out_shape=[
            jax.ShapeDtypeStruct((PHASES, planes * rows, columns), F32),
            jax.ShapeDtypeStruct((SOLUTES, planes * rows, columns), F32),
        ],
        in_specs=[vmem] * (6 + len(halos)),
        out_specs=[hbm, hbm],
        scratch_shapes=[
            field_rows(len(outer[0])),
            field_rows(len(outer[0]) - 2, 1),
            field_rows(len(outer[1])),
            field_rows(len(outer[2])),
            pltpu.VMEM((FIELDS, planes * rows, columns), F32),
            cooling,
            cooling,
            pltpu.SemaphoreType.DMA((2 * len(plan.starts(3, STEPS)),)),
        ],
        cost_estimate=pl.CostEstimate(flops=8_000_000, bytes_accessed=0, transcendentals=0),
        compiler_params=PARAMS,
        name="outer",
    )(*(on_chip(x) for x in (*state, rates, *halos)))
    return (
        phase_out.reshape(PHASES, planes, rows, columns),
        solute_out.reshape(SOLUTES, planes, rows, columns),
    )


def solution(mesh):
    placed = (
        P("grow", "trans", None),
        P("grow", "trans", None),
        P(),
        P(),
        P(None, "grow", "trans", None),
        P(),
    )
    return jax.shard_map(
        shards,
        mesh=mesh,
        in_specs=placed,
        out_specs=(P(None, "grow", "trans", None), P(None, "grow", "trans", None)),
        check_vma=False,
    )
```
